32 devices in a mesh: gx: 4 (over x, core), gy: 2 (over y), gz: 4 (over z).
Axes of the slice: x: 2, y: 2, z: 4, core: 2. Of those that a mesh axis runs over, the one named last changes fastest.
Arguments:
- fields: float32 [5, 64, 16, 512], P(None, 'gz', 'gy', 'gx'), may hold values from -4 to 4
- radius: float32 [8, 64, 16, 512], P(None, 'gz', 'gy', 'gx'), may hold values from 0.4 to 1.5
- weight: float32 [8, 64, 16, 512], P(None, 'gz', 'gy', 'gx'), may hold values from 0.05 to 0.5
- column: int32 [8, 64, 16, 512], P(None, 'gz', 'gy', 'gx'), may hold values from 0 to 127
- counts: int32 [64, 16, 512], P('gz', 'gy', 'gx'), may hold values from 1 to 8
- fall_depth: int32 [8, 64, 16, 4], P(None, 'gz', 'gy', 'gx'), may hold values from 0 to 8, as said below
Outputs:
- new_fields: float32 [5, 64, 16, 512], P(None, 'gz', 'gy', 'gx')
- moments: float32 [3, 64, 16, 512], P(None, 'gz', 'gy', 'gx')
The draws below stay inside these ranges and needn't reach their ends.
Inputs may be any that keep to these rules, and one draw needn't show every extreme that they name: The droplet in slot s of cell (k, j, i) sits in x cell (i // 128) * 128 + column[s, k, j, i]. Slots s < counts[k, j, i] hold live droplets. The droplets of slot s in cells (k, j, b * 128) to (k, j, (b + 1) * 128 - 1) fall together by fall_depth[s, k, j, b] levels, never below the lowest level: fall_depth[s, k, j, b] <= k; 8 is reached in every draw.
All inputs are finite; a program needn't handle non-finite values. Where the reference program divides by a largest or mean magnitude, that divisor is 1e-20 or more.
Results may differ from the reference program's by a relative error of at most 0.00021.
Values sent between devices are 32-bit elements; how exact they have to be, the bound alone decides.
A program may use at most 64 MiB of HBM per device.

```python
import math
import jax
import jax.numpy as jnp
from jax import lax

CX = 128
SLOTS = 8
NS = 4
FMAX = 8
NX = 512
NY = 16
NZ = 64
XBLOCKS = 4


def draw_fall_depth(key, part):
    drawn = jax.random.randint(key, (SLOTS, NZ, NY, XBLOCKS), 0, FMAX + 1, dtype=jnp.int32)
    drawn = drawn.at[0, NZ - 1, 0, 0].set(FMAX)
    levels = jnp.arange(NZ, dtype=jnp.int32)[None, :, None, None]
    return jnp.minimum(drawn, levels).astype(jnp.int32)


def set_ends(values, own_key, least, largest):
    shape = values.shape
    index_at = [jax.random.randint(jax.random.fold_in(own_key, axis), (), 0, shape[axis]) for axis in range(len(shape))]
    values = values.at[tuple(index_at)].set(least)
    longest = shape.index(max(shape))
    index_at[longest] = (index_at[longest] + 1) % shape[longest]
    return values.at[tuple(index_at)].set(largest)


def shard_levels(key, shape, cuts, smallest, high):
    loudness = 1.0
    for position, shards_of in cuts:
        steps = jax.random.uniform(jax.random.fold_in(jax.random.fold_in(key, 6), position), (shards_of,), jnp.float32, smallest / len(cuts), high / len(cuts))
        loudness = loudness * jnp.repeat(jnp.exp(steps), shape[position] // shards_of).reshape((-1,) + (1,) * (len(shape) - 1 - position))
    return loudness


def centred(rng, dims, spread, reach, cuts=(), held_as=jnp.bfloat16):
    entries = spread * jax.random.normal(rng, dims, jnp.float32)
    if cuts:
        entries = entries * shard_levels(rng, dims, cuts, -0.22, 0.18)
    return jnp.clip(entries, -reach, reach).astype(held_as)


def setup_inputs(seed: int = 0) -> dict:
    splits = jax.random.split(jax.random.key(seed), 7)
    fields = centred(splits[0], (5, NZ, NY, NX), 0.5, 4.0, ((1, 4), (2, 2), (3, 4)), jnp.float32)
    radius = jnp.clip(jnp.exp(math.log(1.5) - 1.3217558 * jax.random.uniform(splits[1], (SLOTS, NZ, NY, NX), jnp.float32) ** shard_levels(splits[1], (SLOTS, NZ, NY, NX), ((1, 4), (2, 2), (3, 4)), -0.2, 0.2)), 0.4, 1.5)
    weight = jnp.clip(jnp.exp(math.log(0.5) - 2.3025851 * jax.random.uniform(splits[2], (SLOTS, NZ, NY, NX), jnp.float32) ** shard_levels(splits[2], (SLOTS, NZ, NY, NX), ((1, 4), (2, 2), (3, 4)), -0.2, 0.2)), 0.05, 0.5)
    column = set_ends(jax.random.randint(splits[3], (SLOTS, NZ, NY, NX), 0, CX), jax.random.fold_in(splits[3], 1), 0, CX - 1).astype(jnp.int32)
    counts = set_ends(jax.random.randint(splits[4], (NZ, NY, NX), 1, SLOTS + 1), jax.random.fold_in(splits[4], 1), 1, SLOTS).astype(jnp.int32)
    fall_depth = draw_fall_depth(jax.random.fold_in(splits[6], 71), 0)
    return dict(fields=fields, radius=radius, weight=weight, column=column, counts=counts, fall_depth=fall_depth)


sound_speed = 10.0
buoyancy = 0.5
courant_goal = 0.6
growth = 0.3

def window(padded, margin, direction, offset, length):
    cut = []
    for dimension in range(3):
        if dimension == direction:
            cut.append(slice(margin + offset, margin + offset + length))
        else:
            cut.append(slice(margin, padded.shape[dimension] - margin))
    return padded[tuple(cut)]

def advect(quantity, margin, wind_pad, wind_margin):
    tendency = jnp.zeros(tuple((quantity.shape[dimension] - 2 * margin for dimension in range(3))), jnp.float32)
    for direction in range(3):
        cells_along = quantity.shape[direction] - 2 * margin
        stencil = [window(quantity, margin, direction, offset - 1, cells_along + 1) for offset in range(-2, 4)]
        face_wind = window(wind_pad[2 - direction], wind_margin, direction, -1, cells_along + 1)
        central = 37.0 * (stencil[2] + stencil[3]) - 8.0 * (stencil[1] + stencil[4]) + (stencil[0] + stencil[5])
        upwind = 10.0 * (stencil[3] - stencil[2]) - 5.0 * (stencil[4] - stencil[1]) + (stencil[5] - stencil[0])
        face_flux = (face_wind * central - jnp.abs(face_wind) * upwind) / 60.0
        upper_flux = lax.slice_in_dim(face_flux, 1, cells_along + 1, axis=direction)
        lower_flux = lax.slice_in_dim(face_flux, 0, cells_along, axis=direction)
        tendency = tendency - (upper_flux - lower_flux)
    return tendency

def extend(fields, margin):
    fields = jnp.pad(fields, ((0, 0), (margin, margin), (0, 0), (0, 0)))
    return jnp.pad(fields, ((0, 0), (0, 0), (margin, margin), (margin, margin)), mode='wrap')

def acoustic(fast_fields, lift_term, pressure_rate, sub_step, lid_mask):
    grid_levels, grid_rows, grid_cols = (fast_fields.shape[1], fast_fields.shape[2], fast_fields.shape[3])
    pressure_pad = extend(fast_fields[0:1], 1)[0]
    pressure = fast_fields[0]
    east_wind = fast_fields[1] - sub_step * sound_speed * (window(pressure_pad, 1, 2, 1, grid_cols) - pressure)
    north_wind = fast_fields[2] - sub_step * sound_speed * (window(pressure_pad, 1, 1, 1, grid_rows) - pressure)
    vertical_wind = (fast_fields[3] + sub_step * (lift_term - sound_speed * (window(pressure_pad, 1, 0, 1, grid_levels) - pressure))) * lid_mask
    wind_halo = extend(jnp.stack([east_wind, north_wind, vertical_wind]), 1)
    divergence = east_wind - window(wind_halo[0], 1, 2, -1, grid_cols) + (north_wind - window(wind_halo[1], 1, 1, -1, grid_rows)) + (vertical_wind - window(wind_halo[2], 1, 0, -1, grid_levels))
    pressure = pressure + sub_step * (pressure_rate - sound_speed * divergence)
    return jnp.stack([pressure, east_wind, north_wind, vertical_wind])

def reference(fields, radius, weight, column, counts, fall_depth):
    grid_levels, grid_rows, grid_cols = (fields.shape[1], fields.shape[2], fields.shape[3])
    lid_mask = (jnp.arange(grid_levels, dtype=jnp.int32) < grid_levels - 1).astype(jnp.float32)[:, None, None]
    initial = jnp.concatenate([fields[0:4], (fields[4] * lid_mask)[None]])
    top_speed = jnp.max(jnp.abs(initial[2]) + jnp.abs(initial[3]) + jnp.abs(initial[4]))
    time_step = courant_goal / (1.0 + top_speed)
    current = initial
    for fraction, substeps in ((1.0 / 3.0, 1), (0.5, NS // 2), (1.0, NS)):
        padded = extend(current, 3)
        tracer_rate = advect(padded[0], 3, padded[2:5], 3)
        pressure_rate = advect(padded[1], 3, padded[2:5], 3)
        lift_term = buoyancy * 0.5 * (window(padded[0], 3, 0, 0, grid_levels) + window(padded[0], 3, 0, 1, grid_levels)) * lid_mask
        sub_step = fraction * time_step / substeps
        fast_fields = initial[1:5]
        for repeat in range(substeps):
            fast_fields = acoustic(fast_fields, lift_term, pressure_rate, sub_step, lid_mask)
        tracer = initial[0] + fraction * time_step * tracer_rate
        current = jnp.concatenate([tracer[None], fast_fields])
    tracer = current[0]
    block_start = jnp.arange(grid_cols, dtype=jnp.int32) // CX * CX
    levels = jnp.arange(grid_levels, dtype=jnp.int32)[:, None, None]
    row_index = jnp.arange(grid_rows, dtype=jnp.int32)[None, :, None]
    moments = jnp.zeros((3, grid_levels * grid_rows * grid_cols), jnp.float32)
    for slot_index in range(SLOTS):
        cell_column = (block_start[None, None, :] + column[slot_index]).astype(jnp.int32)
        near_tracer = jnp.take_along_axis(tracer, cell_column, axis=2)
        squared = radius[slot_index] * radius[slot_index] * jnp.exp(growth * near_tracer)
        number = weight[slot_index] * (slot_index < counts).astype(jnp.float32)
        area_term = number * squared
        mass_term = area_term * jnp.sqrt(squared)
        fall_cells = jnp.repeat(fall_depth[slot_index], CX, axis=2).astype(jnp.int32)
        flat_index = (((levels - fall_cells) * grid_rows + row_index) * grid_cols + cell_column).astype(jnp.int32)
        moments = moments.at[:, flat_index.reshape(-1)].add(jnp.stack([number, area_term, mass_term]).reshape(3, -1))
    return (current, moments.reshape(3, grid_levels, grid_rows, grid_cols))
```

```python
import functools
import jax
import jax.numpy as jnp
from jax import lax
from jax.experimental import pallas as pl
from jax.experimental.pallas import tpu as pltpu
from jax.sharding import PartitionSpec as P

NS = 4
FMAX = 8
SLOT_LANES = 8

sound_speed = 10.0
buoyancy = 0.5
courant_goal = 0.6
growth = 0.3

MESH = pl.DeviceIdType.MESH
FULL = {0: 0, 1: 1, 3: 2}
THIN = {2: 0, 4: 1, 5: 2, 6: 3}
AXES = ("gx", "gy", "gz")


def flux(wind, a, b, c, d, e, f):
    central = 37.0 * (c + d) - 8.0 * (b + e) + (a + f)
    upwind = 10.0 * (d - c) - 5.0 * (e - b) + (f - a)
    return wind * central - jnp.abs(wind) * upwind


def kernel(
    sizes, depth_ref, fields, radius_hbm, weight_hbm, column_hbm, counts_hbm,
    out_fields, moments, *scratch
):
    names, levels, rows, cols, slots = sizes
    refs = dict(zip(names, scratch))
    radius, weight, column, counts = (refs[n] for n in ("radius", "weight", "column", "counts"))
    send_sem, recv_sem = refs["send_sem"], refs["recv_sem"]
    shape = (rows, cols)
    lane = lax.broadcasted_iota(jnp.int32, shape, 1)
    row = lax.broadcasted_iota(jnp.int32, shape, 0)
    place = {a: lax.axis_index(a) for a in AXES}
    count = {a: lax.axis_size(a) for a in AXES}
    has_low = place["gz"] > 0
    has_high = place["gz"] < count["gz"] - 1

    def lanes_by(x, shift):
        return pltpu.roll(x, shift % cols if isinstance(shift, int) else shift, 1)

    def rows_by(x, shift):
        return pltpu.roll(x, shift % rows, 0)

    def loop(n, body, carry, unroll=True):
        return lax.fori_loop(0, n, body, carry, unroll=unroll)

    local = []
    for n, (src, dst) in enumerate(
        ((column_hbm, column), (counts_hbm, counts), (weight_hbm, weight), (radius_hbm, radius))
    ):
        copy = pltpu.make_async_copy(src, dst, refs["local_sem"].at[n])
        copy.start()
        local.append(copy)

    barrier = pltpu.get_barrier_semaphore()
    peers = 0
    for a in AXES:
        for step in range(1, count[a]):
            pl.semaphore_signal(
                barrier, inc=1,
                device_id={a: lax.rem(place[a] + step, count[a])}, device_id_type=MESH,
            )
            peers += 1

    def first(k, top):
        w = fields[4, k]
        lid = jnp.where((k == levels - 1) & jnp.logical_not(has_high), 0.0, 1.0)
        w = w * lid
        refs["W0"][k + 1] = w
        refs["C0"][k + 3] = fields[0, k]
        refs["P0"][k + 3] = fields[1, k]
        refs["U0"][k] = fields[2, k]
        refs["V0"][k] = fields[3, k]
        return jnp.maximum(top, jnp.abs(fields[2, k]) + jnp.abs(fields[3, k]) + jnp.abs(w))

    top = loop(levels, first, jnp.zeros(shape, jnp.float32))
    pl.semaphore_wait(barrier, peers)

    def max_start(phase, value):
        a = AXES[phase]
        refs["max_send"][phase] = value
        copies = []
        for step in range(1, count[a]):
            copy = pltpu.make_async_remote_copy(
                src_ref=refs["max_send"].at[phase],
                dst_ref=refs["max_recv"].at[phase, step - 1],
                send_sem=refs["max_ss"].at[phase, step - 1],
                recv_sem=refs["max_rs"].at[phase, step - 1],
                device_id={a: lax.rem(place[a] + step, count[a])}, device_id_type=MESH,
            )
            copy.start()
            copies.append(copy)
        return copies

    def max_end(phase, value, copies):
        for n, copy in enumerate(copies):
            copy.wait()
            value = jnp.maximum(value, refs["max_recv"][phase, n])
        return value

    def neighbour(a, step):
        return {a: lax.rem(place[a] + count[a] + step, count[a])}

    def copies_of(e):
        kind, at = ("f", FULL[e]) if e in FULL else ("t", THIN[e])
        out = {}
        for n, (name, a, step) in enumerate(
            (("yu", "gy", 1), ("yd", "gy", -1), ("zu", "gz", 1), ("zd", "gz", -1),
             ("xu", "gx", 1), ("xd", "gx", -1))
        ):
            out[name] = pltpu.make_async_remote_copy(
                src_ref=refs[kind + name + "_s"].at[at],
                dst_ref=refs[kind + name + "_r"].at[at],
                send_sem=send_sem.at[e, n],
                recv_sem=recv_sem.at[e, n],
                device_id=neighbour(a, step), device_id_type=MESH,
            )
        return out

    def send(e, tag):
        full = e in FULL
        kind, at = ("f", FULL[e]) if full else ("t", THIN[e])
        C, PR, U, V, W = (refs[n + tag] for n in "CPUVW")
        copies = copies_of(e)

        def pack_y(k, carry):
            p, v = PR[k + 3], V[k]
            if full:
                c = C[k + 3]
                refs["fyu_s"][at, k] = jnp.where(
                    row >= rows - 3, c, jnp.where(row == rows - 4, rows_by(v, -3), rows_by(p, -4))
                )
                refs["fyd_s"][at, k] = jnp.where(row < 3, c, rows_by(p, 3))
            else:
                refs["tyu_s"][at, pl.ds(k, 1), :] = p[rows - 1:rows]
                refs["tyu_s"][at, pl.ds(levels + k, 1), :] = v[rows - 1:rows]
                refs["tyd_s"][at, pl.ds(k, 1), :] = p[0:1]
            return carry

        loop(levels, pack_y, 0)
        width = 3 if full else 1
        for t in range(width):
            top_level = levels - width + t
            if full:
                refs["fzu_s"][at, t] = C[3 + top_level]
                refs["fzd_s"][at, t] = C[3 + t]
                refs["fzu_s"][at, 3 + t] = PR[3 + top_level]
                refs["fzd_s"][at, 3 + t] = PR[3 + t]
            else:
                refs["tzu_s"][at, 0] = PR[3 + top_level]
                refs["tzd_s"][at, 0] = PR[3]
        refs[kind + "zu_s"][at, 6 if full else 1] = W[levels]
        copies["yu"].start()
        copies["yd"].start()

        def pack_x(k, carry):
            up, down = carry
            p, u = PR[k + 3], U[k]
            if full:
                c = C[k + 3]
                high = jnp.where(
                    lane >= cols - 3, c,
                    jnp.where(lane == cols - 4, lanes_by(u, -3), lanes_by(p, -4)),
                )
                low = jnp.where(lane < 3, c, lanes_by(p, 3))
            else:
                high = jnp.where(lane == cols - 4, lanes_by(u, -3), lanes_by(p, -4))
                low = lanes_by(p, 3)
            here = lane // SLOT_LANES == k
            up = jnp.where(here, lanes_by(high, lax.rem(SLOT_LANES * (k + 1), cols)), up)
            down = jnp.where(here, lanes_by(low, SLOT_LANES * k), down)
            return up, down

        zero = jnp.zeros(shape, jnp.float32)
        up, down = loop(levels, pack_x, (zero, zero))
        refs[kind + "xu_s"][at] = up
        refs[kind + "xd_s"][at] = down

        @pl.when(has_high)
        def _():
            copies["zu"].start()

        @pl.when(has_low)
        def _():
            copies["zd"].start()

        copies["xu"].start()
        copies["xd"].start()

    def receive(e, tag):
        full = e in FULL
        kind, at = ("f", FULL[e]) if full else ("t", THIN[e])
        C, PR, W = (refs[n + tag] for n in "CPW")
        copies = copies_of(e)
        width = 3 if full else 1

        copies["xu"].wait()
        copies["xd"].wait()
        up, down = refs[kind + "xu_r"][at], refs[kind + "xd_r"][at]

        def unpack_x(k, carry):
            low = lanes_by(up, cols - SLOT_LANES * (k + 1))
            high = lanes_by(down, (cols - SLOT_LANES * k) % cols)
            if full:
                refs["HXC" + tag][k] = jnp.where(lane >= cols - 3, low, high)
            refs["HXP" + tag][k] = jnp.where(lane >= cols - 3, lanes_by(low, 4), lanes_by(high, -3))
            refs["HXU" + tag][k] = lanes_by(low, 3)
            return carry

        loop(levels, unpack_x, 0)

        @pl.when(has_high)
        def _():
            copies["zu"].wait_send()
            copies["zd"].wait_recv()
            for t in range(width):
                if full:
                    C[3 + levels + t] = refs["fzd_r"][at, t]
                    PR[3 + levels + t] = refs["fzd_r"][at, 3 + t]
                else:
                    PR[3 + levels + t] = refs["tzd_r"][at, t]

        @pl.when(jnp.logical_not(has_high))
        def _():
            for t in range(width):
                if full:
                    C[3 + levels + t] = jnp.zeros(shape, jnp.float32)
                PR[3 + levels + t] = jnp.zeros(shape, jnp.float32)

        @pl.when(has_low)
        def _():
            copies["zd"].wait_send()
            copies["zu"].wait_recv()
            for t in range(width):
                if full:
                    C[t] = refs["fzu_r"][at, t]
                    PR[t] = refs["fzu_r"][at, 3 + t]
                else:
                    PR[2] = refs["tzu_r"][at, 0]
            W[0] = refs[kind + "zu_r"][at, 6 if full else 1]

        @pl.when(jnp.logical_not(has_low))
        def _():
            for t in range(width):
                if full:
                    C[t] = jnp.zeros(shape, jnp.float32)
                PR[3 - width + t] = jnp.zeros(shape, jnp.float32)
            W[0] = jnp.zeros(shape, jnp.float32)

        copies["yu"].wait()
        copies["yd"].wait()

        def unpack_y(k, carry):
            if full:
                low, high = refs["fyu_r"][at, k], refs["fyd_r"][at, k]
                refs["HYC" + tag][k] = jnp.where(row >= rows - 3, low, high)
                refs["HYP" + tag][k] = jnp.where(row >= rows - 3, rows_by(low, 4), rows_by(high, -3))
                refs["HYV" + tag][k] = rows_by(low, 3)
            else:
                low = refs["tyu_r"][at, pl.ds(k, 1), :]
                high = refs["tyd_r"][at, pl.ds(k, 1), :]
                refs["HYP" + tag][k] = jnp.where(row == rows - 1, low, high)
                refs["HYV" + tag][k] = jnp.broadcast_to(
                    refs["tyu_r"][at, pl.ds(levels + k, 1), :], shape
                )
            return carry

        loop(levels, unpack_y, 0)

    def sides(q, halo, by, index, extent):
        low = [by(jnp.where(index >= extent - n, halo, q), n) for n in (3, 2, 1)]
        high = [by(jnp.where(index < n, halo, q), -n) for n in (1, 2, 3)]
        return (*low, q, *high)

    def advect(tag):
        U, V, W = (refs[n + tag] for n in "UVW")

        def level(k, carry):
            u, v, w, w_low = U[k], V[k], W[k + 1], W[k]
            u_low = lanes_by(jnp.where(lane == cols - 1, refs["HXU" + tag][k], u), 1)
            v_low = rows_by(jnp.where(row == rows - 1, refs["HYV" + tag][k], v), 1)
            for name, rate in (("C", "rate_c"), ("P", "rate_p")):
                Q = refs[name + tag]
                q = Q[k + 3]
                xs = sides(q, refs["HX" + name + tag][k], lanes_by, lane, cols)
                ys = sides(q, refs["HY" + name + tag][k], rows_by, row, rows)
                zs = [Q[k + n] for n in range(7)]
                total = flux(u, *xs[1:]) - flux(u_low, *xs[:6])
                total = total + (flux(v, *ys[1:]) - flux(v_low, *ys[:6]))
                total = total + (flux(w, *zs[1:]) - flux(w_low, *zs[:6]))
                refs[rate][k] = total * (-1.0 / 60.0)
            return carry

        loop(levels, level, 0, 4)
        C = refs["C" + tag]
        lid_low = jnp.where(has_low, 1.0, 0.0)
        lid_high = jnp.where(has_high, 1.0, 0.0)
        for k in range(levels + 1):
            lift = (buoyancy * 0.5) * (C[k + 2] + C[k + 3])
            if k == 0:
                lift = lift * lid_low
            if k == levels:
                lift = lift * lid_high
            refs["lift"][k] = lift

    def substep(source, sub_step):
        SP, SU, SV, SW = (refs[n + source] for n in "PUVW")
        HXP, HXU, HYP, HYV = (refs[n + source] for n in ("HXP", "HXU", "HYP", "HYV"))
        DP, DU, DV, DW = (refs[n + "1"] for n in "PUVW")
        push = sub_step * sound_speed
        lid_low = jnp.where(has_low, 1.0, 0.0)

        def vertical(k):
            return SW[k] + sub_step * (
                refs["lift"][k] - sound_speed * (SP[k + 3] - SP[k + 2])
            )

        def level(k, w_low):
            p, u, v = SP[k + 3], SU[k], SV[k]
            hx, hy = HXP[k], HYP[k]
            lid = jnp.where((k == levels - 1) & jnp.logical_not(has_high), 0.0, 1.0)
            w = vertical(k + 1) * lid
            px = lanes_by(p, -1)
            py = rows_by(p, -1)
            u_new = u - push * (jnp.where(lane == cols - 1, lanes_by(hx, -1), px) - p)
            v_new = v - push * (jnp.where(row == rows - 1, rows_by(hy, -1), py) - p)
            u_halo = HXU[k] - push * (px - hx)
            v_halo = HYV[k] - push * (py - hy)
            u_low = lanes_by(jnp.where(lane == cols - 1, u_halo, u_new), 1)
            v_low = rows_by(jnp.where(row == rows - 1, v_halo, v_new), 1)
            div = (u_new - u_low) + (v_new - v_low) + (w - w_low)
            DU[k] = u_new
            DV[k] = v_new
            DW[k + 1] = w
            DP[k + 3] = p + sub_step * (refs["rate_p"][k] - sound_speed * div)
            return w

        loop(levels, level, vertical(0) * lid_low)

    def tracer(scale):
        def level(k, carry):
            refs["C1"][k + 3] = refs["C0"][k + 3] + scale * refs["rate_c"][k]
            return carry

        loop(levels, level, 0)

    acc, vals = refs["acc"], refs["vals"]

    def growth_terms():
        for n in range(4):
            local[n].wait()

        def cell(k, carry):
            c = refs["C1"][k + 3]
            live = counts[k]
            for s in range(slots):
                near = jnp.take_along_axis(c, column[s, k], axis=1, mode="promise_in_bounds")
                r = radius[s, k]
                squared = r * r * jnp.exp(growth * near)
                number = jnp.where(live > s, weight[s, k], 0.0)
                area = number * squared
                mass = area * jnp.sqrt(squared)
                for m, term in enumerate((number, area, mass)):
                    high = term.astype(jnp.bfloat16).astype(jnp.float32)
                    vals[s, k, m * rows:(m + 1) * rows, :] = high
                    vals[s, k, (m + 3) * rows:(m + 4) * rows, :] = term - high
                vals[s, k, 6 * rows:, :] = jnp.zeros((2 * rows, cols), jnp.float32)
            return carry

        loop(levels, cell, 0, 2)

    def clear():
        def level(k, carry):
            acc[k] = jnp.zeros((8 * rows, cols), jnp.float32)
            return carry

        loop(levels + FMAX, level, 0)

    def deposit(begin, end):
        ids = lax.broadcasted_iota(jnp.int32, (cols, cols), 0).astype(jnp.float32).astype(jnp.bfloat16)
        one = jnp.ones((cols, cols), jnp.bfloat16)
        none = jnp.zeros((cols, cols), jnp.bfloat16)
        zero = jnp.zeros((8, cols), jnp.float32)

        def cell(n, carry):
            k, j = begin + n // rows, n % rows
            by_depth = [None] * (FMAX + 1)
            for s in range(0, slots, 2):
                left, right, hots = [], [], []
                for t in range(2):
                    v = vals[s + t, k, pl.ds(j, 8, stride=rows), :]
                    left.append(v if t == 0 else zero)
                    right.append(zero if t == 0 else v)
                    c = column[s + t, k, pl.ds(j, 1), :].astype(jnp.float32).astype(jnp.bfloat16)
                    hots.append(jnp.where(ids == jnp.broadcast_to(c, (cols, cols)), one, none))
                lhs = jnp.concatenate(
                    [jnp.concatenate(left, axis=0), jnp.concatenate(right, axis=0)], axis=1
                ).astype(jnp.bfloat16)
                rhs = jnp.concatenate(hots, axis=1)
                got = lax.dot_general(
                    lhs, rhs, (((1,), (1,)), ((), ())), preferred_element_type=jnp.float32
                )
                for t in range(2):
                    part = got[8 * t:8 * (t + 1)]
                    depth = depth_ref[s + t, k * rows + j]
                    for d in range(FMAX + 1):
                        term = jnp.where(depth == d, part, 0.0)
                        by_depth[d] = term if by_depth[d] is None else by_depth[d] + term
            for d in range(FMAX + 1):
                at = pl.ds(pl.multiple_of(j * 8, 8), 8)
                acc[k + FMAX - d, at, :] = acc[k + FMAX - d, at, :] + by_depth[d]
            return carry

        lax.fori_loop(0, (end - begin) * rows, cell, 0, unroll=2)

    def collect(m, l):
        return acc[l, pl.ds(m, rows, stride=8), :] + acc[l, pl.ds(m + 3, rows, stride=8), :]

    copies = max_start(0, top)
    send(0, "0")
    top = max_end(0, top, copies)
    copies = max_start(1, top)
    top = max_end(1, top, copies)
    copies = max_start(2, top)
    clear()
    receive(0, "0")
    advect("0")
    top = max_end(2, top, copies)
    time_step = courant_goal / (1.0 + jnp.max(top, axis=(0, 1), keepdims=True))
    time_step = jnp.broadcast_to(time_step, shape)

    third = time_step * (1.0 / 3.0)
    tracer(third)
    substep("0", third)
    send(1, "1")
    receive(1, "1")
    advect("1")
    half = time_step * 0.5
    tracer(half)
    part = half / (NS // 2)
    substep("0", part)
    send(2, "1")
    receive(2, "1")
    substep("1", part)
    send(3, "1")
    receive(3, "1")
    advect("1")
    tracer(time_step)
    part = time_step / NS
    substep("0", part)
    send(4, "1")
    growth_terms()
    receive(4, "1")
    substep("1", part)
    send(5, "1")
    deposit(0, FMAX)
    moment_copy = pltpu.make_async_remote_copy(
        src_ref=refs["fall_s"], dst_ref=refs["fall_r"],
        send_sem=refs["fall_sem"].at[0], recv_sem=refs["fall_sem"].at[1],
        device_id=neighbour("gz", -1), device_id_type=MESH,
    )
    for m in range(3):
        for l in range(FMAX):
            refs["fall_s"][m, l] = collect(m, l)

    receive(5, "1")

    @pl.when(has_low)
    def _():
        moment_copy.start()

    substep("1", part)
    send(6, "1")
    deposit(FMAX, levels)
    receive(6, "1")
    substep("1", part)

    def write(k, carry):
        out_fields[0, k] = refs["C1"][k + 3]
        out_fields[1, k] = refs["P1"][k + 3]
        out_fields[2, k] = refs["U1"][k]
        out_fields[3, k] = refs["V1"][k]
        out_fields[4, k] = refs["W1"][k + 1]
        return carry

    loop(levels, write, 0)
    for m in range(3):
        for l in range(levels):
            moments[m, l] = collect(m, l + FMAX)

    @pl.when(has_low)
    def _():
        moment_copy.wait_send()

    @pl.when(has_high)
    def _():
        moment_copy.wait_recv()
        for m in range(3):
            for l in range(FMAX):
                at = levels - FMAX + l
                moments[m, at] = moments[m, at] + refs["fall_r"][m, l]


def per_device(fields, radius, weight, column, counts, fall_depth):
    levels, rows, cols = fields.shape[1:]
    slots = radius.shape[0]
    assert levels * SLOT_LANES <= cols and rows == 8 and FMAX <= levels
    f32 = jnp.float32
    cell = (rows, cols)
    widest = max(lax.axis_size(a) for a in AXES) - 1
    spaces = {}

    def add(name, *shape, dtype=f32):
        spaces[name] = pltpu.VMEM(shape, dtype)

    add("radius", *radius.shape)
    add("weight", *weight.shape)
    add("column", *column.shape, dtype=jnp.int32)
    add("counts", *counts.shape, dtype=jnp.int32)
    for tag in "01":
        add("C" + tag, levels + 6, *cell)
        add("P" + tag, levels + 6, *cell)
        add("U" + tag, levels, *cell)
        add("V" + tag, levels, *cell)
        add("W" + tag, levels + 1, *cell)
        for name in ("HXC", "HXP", "HXU", "HYC", "HYP", "HYV"):
            add(name + tag, levels, *cell)
    add("rate_c", levels, *cell)
    add("rate_p", levels, *cell)
    add("lift", levels + 1, *cell)
    add("max_send", 3, *cell)
    add("max_recv", 3, widest, *cell)
    for end in ("_s", "_r"):
        for name, shape in (
            ("fxu", cell), ("fxd", cell), ("fyu", (levels,) + cell), ("fyd", (levels,) + cell),
            ("fzu", (7,) + cell), ("fzd", (6,) + cell),
        ):
            add(name + end, len(FULL), *shape)
        for name, shape in (
            ("txu", cell), ("txd", cell), ("tyu", (2 * levels, cols)), ("tyd", (levels, cols)),
            ("tzu", (2,) + cell), ("tzd", (1,) + cell),
        ):
            add(name + end, len(THIN), *shape)
    add("acc", levels + FMAX, 8 * rows, cols)
    add("vals", slots, levels, 8 * rows, cols)
    add("fall_s", 3, FMAX, *cell)
    add("fall_r", 3, FMAX, *cell)
    rounds = len(FULL) + len(THIN)
    spaces["send_sem"] = pltpu.SemaphoreType.DMA((rounds, 6))
    spaces["recv_sem"] = pltpu.SemaphoreType.DMA((rounds, 6))
    spaces["max_ss"] = pltpu.SemaphoreType.DMA((3, widest))
    spaces["max_rs"] = pltpu.SemaphoreType.DMA((3, widest))
    spaces["fall_sem"] = pltpu.SemaphoreType.DMA((2,))
    spaces["local_sem"] = pltpu.SemaphoreType.DMA((4,))
    vmem = pl.BlockSpec(memory_space=pltpu.VMEM)
    anywhere = pl.BlockSpec(memory_space=pl.ANY)
    return pl.pallas_call(
        functools.partial(kernel, (tuple(spaces), levels, rows, cols, slots)),
        out_shape=(
            jax.ShapeDtypeStruct(fields.shape, f32),
            jax.ShapeDtypeStruct((3, levels, rows, cols), f32),
        ),
        in_specs=[pl.BlockSpec(memory_space=pltpu.SMEM), vmem] + [anywhere] * 4,
        out_specs=(vmem, vmem),
        scratch_shapes=list(spaces.values()),
        compiler_params=pltpu.CompilerParams(
            collective_id=0, has_side_effects=True, vmem_limit_bytes=48 * 1024 * 1024
        ),
        name="slab_step",
    )(fall_depth.reshape(slots, levels * rows), fields, radius, weight, column, counts)


def solution(mesh):
    in_specs = (
        P(None, "gz", "gy", "gx"),
        P(None, "gz", "gy", "gx"),
        P(None, "gz", "gy", "gx"),
        P(None, "gz", "gy", "gx"),
        P("gz", "gy", "gx"),
        P(None, "gz", "gy", "gx"),
    )
    out_specs = (P(None, "gz", "gy", "gx"), P(None, "gz", "gy", "gx"))
    return jax.shard_map(
        per_device, mesh=mesh, in_specs=in_specs, out_specs=out_specs, check_vma=False
    )
```

```python
import functools
import jax
import jax.numpy as jnp
from jax import lax
from jax.experimental import pallas as pl
from jax.experimental.pallas import tpu as pltpu
from jax.sharding import PartitionSpec as P

NS = 4
FMAX = 8
CELLS = 8
SLOT_LANES = 8

sound_speed = 10.0
buoyancy = 0.5
courant_goal = 0.6
growth = 0.3

MESH = pl.DeviceIdType.MESH
FULL = {0: 0, 1: 1, 3: 2}
THIN = {2: 0, 4: 1, 5: 2, 6: 3}
AXES = ("gy", "gx", "gz")


def flux(wind, a, b, c, d, e, f):
    central = 37.0 * (c + d) - 8.0 * (b + e) + (a + f)
    upwind = 10.0 * (d - c) - 5.0 * (e - b) + (f - a)
    return wind * central - jnp.abs(wind) * upwind


def kernel(
    sizes, depth_ref, fields_hbm, radius_hbm, weight_hbm, column_hbm, counts_hbm,
    out_fields, moments, *scratch
):
    names, levels, rows, cols, slots = sizes
    refs = dict(zip(names, scratch))
    radius, weight, column, counts = (refs[n] for n in ("radius", "weight", "column", "counts"))
    fields = refs["fields"]
    send_sem, recv_sem = refs["send_sem"], refs["recv_sem"]
    shape = (rows, cols)
    lane = lax.broadcasted_iota(jnp.int32, shape, 1)
    row = lax.broadcasted_iota(jnp.int32, shape, 0)
    place = {a: lax.axis_index(a) for a in AXES}
    count = {a: lax.axis_size(a) for a in AXES}
    has_low = place["gz"] > 0
    has_high = place["gz"] < count["gz"] - 1

    def lanes_by(x, shift):
        return pltpu.roll(x, shift % cols if isinstance(shift, int) else shift, 1)

    def rows_by(x, shift):
        return pltpu.roll(x, shift % rows, 0)

    def loop(n, body, carry, unroll=True):
        return lax.fori_loop(0, n, body, carry, unroll=unroll)

    fields_copy = pltpu.make_async_copy(fields_hbm, fields, refs["local_sem"].at[4])
    fields_copy.start()
    local = []
    for n, (src, dst) in enumerate(
        ((column_hbm, column), (counts_hbm, counts), (weight_hbm, weight), (radius_hbm, radius))
    ):
        copy = pltpu.make_async_copy(src, dst, refs["local_sem"].at[n])
        copy.start()
        local.append(copy)

    barrier = pltpu.get_barrier_semaphore()
    peers = 0
    for a in AXES:
        for step in range(1, count[a]):
            pl.semaphore_signal(
                barrier, inc=1,
                device_id={a: lax.rem(place[a] + step, count[a])}, device_id_type=MESH,
            )
            peers += 1

    fields_copy.wait()

    def first(k, top):
        w = fields[4, k]
        lid = jnp.where((k == levels - 1) & jnp.logical_not(has_high), 0.0, 1.0)
        w = w * lid
        refs["W0"][k + 1] = w
        refs["C0"][k + 3] = fields[0, k]
        refs["P0"][k + 3] = fields[1, k]
        refs["U0"][k] = fields[2, k]
        refs["V0"][k] = fields[3, k]
        return jnp.maximum(top, jnp.abs(fields[2, k]) + jnp.abs(fields[3, k]) + jnp.abs(w))

    top = loop(levels, first, jnp.zeros(shape, jnp.float32))
    pl.semaphore_wait(barrier, peers)

    def max_start(phase, value):
        a = AXES[phase]
        refs["max_send"][phase] = value
        copies = []
        for step in range(1, count[a]):
            copy = pltpu.make_async_remote_copy(
                src_ref=refs["max_send"].at[phase],
                dst_ref=refs["max_recv"].at[phase, step - 1],
                send_sem=refs["max_ss"].at[phase, step - 1],
                recv_sem=refs["max_rs"].at[phase, step - 1],
                device_id={a: lax.rem(place[a] + step, count[a])}, device_id_type=MESH,
            )
            copy.start()
            copies.append(copy)
        return copies

    def max_end(phase, value, copies):
        for n, copy in enumerate(copies):
            copy.wait()
            value = jnp.maximum(value, refs["max_recv"][phase, n])
        return value

    def neighbour(a, step):
        return {a: lax.rem(place[a] + count[a] + step, count[a])}

    def copies_of(e, wanted=("yu", "yd", "zu", "zd", "xu", "xd")):
        kind, at = ("f", FULL[e]) if e in FULL else ("t", THIN[e])
        out = {}
        for n, (name, a, step) in enumerate(
            (("yu", "gy", 1), ("yd", "gy", -1), ("zu", "gz", 1), ("zd", "gz", -1),
             ("xu", "gx", 1), ("xd", "gx", -1))
        ):
            if name not in wanted:
                continue
            out[name] = pltpu.make_async_remote_copy(
                src_ref=refs[kind + name + "_s"].at[at],
                dst_ref=refs[kind + name + "_r"].at[at],
                send_sem=send_sem.at[e, n],
                recv_sem=recv_sem.at[e, n],
                device_id=neighbour(a, step), device_id_type=MESH,
            )
        return out

    def send(e, tag):
        full = e in FULL
        kind, at = ("f", FULL[e]) if full else ("t", THIN[e])
        C, PR, U, V, W = (refs[n + tag] for n in "CPUVW")
        copies = copies_of(e)

        def pack_y(k, carry):
            p, v = PR[k + 3], V[k]
            if full:
                c = C[k + 3]
                refs["fyu_s"][at, k] = jnp.where(
                    row >= rows - 3, c, jnp.where(row == rows - 4, rows_by(v, -3), rows_by(p, -4))
                )
                refs["fyd_s"][at, k] = jnp.where(row < 3, c, rows_by(p, 3))
            else:
                refs["tyu_s"][at, pl.ds(k, 1), :] = p[rows - 1:rows]
                refs["tyu_s"][at, pl.ds(levels + k, 1), :] = v[rows - 1:rows]
                refs["tyd_s"][at, pl.ds(k, 1), :] = p[0:1]
            return carry

        loop(levels, pack_y, 0)
        width = 3 if full else 1
        for t in range(width):
            top_level = levels - width + t
            if full:
                refs["fzu_s"][at, t] = C[3 + top_level]
                refs["fzd_s"][at, t] = C[3 + t]
                refs["fzu_s"][at, 3 + t] = PR[3 + top_level]
                refs["fzd_s"][at, 3 + t] = PR[3 + t]
            else:
                refs["tzu_s"][at, 0] = PR[3 + top_level]
                refs["tzd_s"][at, 0] = PR[3]
        refs[kind + "zu_s"][at, 6 if full else 1] = W[levels]
        copies["yu"].start()
        copies["yd"].start()

        def pack_x(k, carry):
            up, down = carry
            p, u = PR[k + 3], U[k]
            if full:
                c = C[k + 3]
                high = jnp.where(
                    lane >= cols - 3, c,
                    jnp.where(lane == cols - 4, lanes_by(u, -3), lanes_by(p, -4)),
                )
                low = jnp.where(lane < 3, c, lanes_by(p, 3))
            else:
                high = jnp.where(lane == cols - 4, lanes_by(u, -3), lanes_by(p, -4))
                low = lanes_by(p, 3)
            here = lane // SLOT_LANES == k
            up = jnp.where(here, lanes_by(high, lax.rem(SLOT_LANES * (k + 1), cols)), up)
            down = jnp.where(here, lanes_by(low, SLOT_LANES * k), down)
            return up, down

        zero = jnp.zeros(shape, jnp.float32)
        up, down = loop(levels, pack_x, (zero, zero))
        refs[kind + "xu_s"][at] = up
        refs[kind + "xd_s"][at] = down

        @pl.when(has_high)
        def _():
            copies["zu"].start()

        @pl.when(has_low)
        def _():
            copies["zd"].start()

        copies["xu"].start()
        copies["xd"].start()

    def receive(e, tag):
        full = e in FULL
        kind, at = ("f", FULL[e]) if full else ("t", THIN[e])
        C, PR, W = (refs[n + tag] for n in "CPW")
        copies = copies_of(e, ("xu", "xd", "zu", "zd"))
        width = 3 if full else 1

        copies["xu"].wait()
        copies["xd"].wait()
        up, down = refs[kind + "xu_r"][at], refs[kind + "xd_r"][at]

        def unpack_x(k, carry):
            low = lanes_by(up, cols - SLOT_LANES * (k + 1))
            high = lanes_by(down, (cols - SLOT_LANES * k) % cols)
            if full:
                refs["HXC" + tag][k] = jnp.where(lane >= cols - 3, low, high)
            refs["HXP" + tag][k] = jnp.where(lane >= cols - 3, lanes_by(low, 4), lanes_by(high, -3))
            refs["HXU" + tag][k] = lanes_by(low, 3)
            return carry

        loop(levels, unpack_x, 0)

        @pl.when(has_high)
        def _():
            copies["zu"].wait_send()
            copies["zd"].wait_recv()
            for t in range(width):
                if full:
                    C[3 + levels + t] = refs["fzd_r"][at, t]
                    PR[3 + levels + t] = refs["fzd_r"][at, 3 + t]
                else:
                    PR[3 + levels + t] = refs["tzd_r"][at, t]

        @pl.when(jnp.logical_not(has_high))
        def _():
            for t in range(width):
                if full:
                    C[3 + levels + t] = jnp.zeros(shape, jnp.float32)
                PR[3 + levels + t] = jnp.zeros(shape, jnp.float32)

        @pl.when(has_low)
        def _():
            copies["zd"].wait_send()
            copies["zu"].wait_recv()
            for t in range(width):
                if full:
                    C[t] = refs["fzu_r"][at, t]
                    PR[t] = refs["fzu_r"][at, 3 + t]
                else:
                    PR[2] = refs["tzu_r"][at, 0]
            W[0] = refs[kind + "zu_r"][at, 6 if full else 1]

        @pl.when(jnp.logical_not(has_low))
        def _():
            for t in range(width):
                if full:
                    C[t] = jnp.zeros(shape, jnp.float32)
                PR[3 - width + t] = jnp.zeros(shape, jnp.float32)
            W[0] = jnp.zeros(shape, jnp.float32)

    def receive_y(e, tag):
        full = e in FULL
        at = FULL[e] if full else THIN[e]
        copies = copies_of(e, ("yu", "yd"))
        copies["yu"].wait()
        copies["yd"].wait()

        def unpack_y(k, carry):
            if full:
                low, high = refs["fyu_r"][at, k], refs["fyd_r"][at, k]
                refs["HYC" + tag][k] = jnp.where(row >= rows - 3, low, high)
                refs["HYP" + tag][k] = jnp.where(row >= rows - 3, rows_by(low, 4), rows_by(high, -3))
                refs["HYV" + tag][k] = rows_by(low, 3)
            else:
                low = refs["tyu_r"][at, pl.ds(k, 1), :]
                high = refs["tyd_r"][at, pl.ds(k, 1), :]
                refs["HYP" + tag][k] = jnp.where(row == rows - 1, low, high)
                refs["HYV" + tag][k] = jnp.broadcast_to(
                    refs["tyu_r"][at, pl.ds(levels + k, 1), :], shape
                )
            return carry

        loop(levels, unpack_y, 0)

    def sides(q, halo, by, index, extent):
        low = [by(jnp.where(index >= extent - n, halo, q), n) for n in (3, 2, 1)]
        high = [by(jnp.where(index < n, halo, q), -n) for n in (1, 2, 3)]
        return (*low, q, *high)

    def advect(tag, along_y):
        U, V, W = (refs[n + tag] for n in "UVW")

        def level(k, carry):
            u, w, w_low = U[k], W[k + 1], W[k]
            u_low = lanes_by(jnp.where(lane == cols - 1, refs["HXU" + tag][k], u), 1)
            for name, rate in (("C", "rate_c"), ("P", "rate_p")):
                Q = refs[name + tag]
                xs = sides(Q[k + 3], refs["HX" + name + tag][k], lanes_by, lane, cols)
                zs = [Q[k + n] for n in range(7)]
                total = flux(u, *xs[1:]) - flux(u_low, *xs[:6])
                refs[rate][k] = total + (flux(w, *zs[1:]) - flux(w_low, *zs[:6]))
            return carry

        def level_y(k, carry):
            v = V[k]
            v_low = rows_by(jnp.where(row == rows - 1, refs["HYV" + tag][k], v), 1)
            for name, rate in (("C", "rate_c"), ("P", "rate_p")):
                ys = sides(refs[name + tag][k + 3], refs["HY" + name + tag][k], rows_by, row, rows)
                total = refs[rate][k] + (flux(v, *ys[1:]) - flux(v_low, *ys[:6]))
                refs[rate][k] = total * (-1.0 / 60.0)
            return carry

        if along_y:
            loop(levels, level_y, 0, 8)
            return
        loop(levels, level, 0, 8)
        C = refs["C" + tag]
        lid_low = jnp.where(has_low, 1.0, 0.0)
        lid_high = jnp.where(has_high, 1.0, 0.0)
        for k in range(levels + 1):
            lift = (buoyancy * 0.5) * (C[k + 2] + C[k + 3])
            if k == 0:
                lift = lift * lid_low
            if k == levels:
                lift = lift * lid_high
            refs["lift"][k] = lift

    def substep(source, sub_step):
        SP, SU, SV, SW = (refs[n + source] for n in "PUVW")
        HXP, HXU, HYP, HYV = (refs[n + source] for n in ("HXP", "HXU", "HYP", "HYV"))
        DP, DU, DV, DW = (refs[n + "1"] for n in "PUVW")
        push = sub_step * sound_speed
        lid_low = jnp.where(has_low, 1.0, 0.0)

        def vertical(k):
            return SW[k] + sub_step * (
                refs["lift"][k] - sound_speed * (SP[k + 3] - SP[k + 2])
            )

        def level(k, w_low):
            p, u, v = SP[k + 3], SU[k], SV[k]
            hx, hy = HXP[k], HYP[k]
            lid = jnp.where((k == levels - 1) & jnp.logical_not(has_high), 0.0, 1.0)
            w = vertical(k + 1) * lid
            px = lanes_by(p, -1)
            py = rows_by(p, -1)
            u_new = u - push * (jnp.where(lane == cols - 1, lanes_by(hx, -1), px) - p)
            v_new = v - push * (jnp.where(row == rows - 1, rows_by(hy, -1), py) - p)
            u_halo = HXU[k] - push * (px - hx)
            v_halo = HYV[k] - push * (py - hy)
            u_low = lanes_by(jnp.where(lane == cols - 1, u_halo, u_new), 1)
            v_low = rows_by(jnp.where(row == rows - 1, v_halo, v_new), 1)
            div = (u_new - u_low) + (v_new - v_low) + (w - w_low)
            DU[k] = u_new
            DV[k] = v_new
            DW[k + 1] = w
            DP[k + 3] = p + sub_step * (refs["rate_p"][k] - sound_speed * div)
            return w

        loop(levels, level, vertical(0) * lid_low)

    def tracer(scale):
        def level(k, carry):
            refs["C1"][k + 3] = refs["C0"][k + 3] + scale * refs["rate_c"][k]
            return carry

        loop(levels, level, 0)

    acc, vals = refs["acc"], refs["vals"]

    def growth_terms():
        for n in range(4):
            local[n].wait()

        def cell(k, carry):
            c = refs["C1"][k + 3]
            live = counts[k]
            for s in range(slots):
                near = jnp.take_along_axis(c, column[s, k], axis=1, mode="promise_in_bounds")
                r = radius[s, k]
                squared = r * r * jnp.exp(growth * near)
                number = jnp.where(live > s, weight[s, k], 0.0)
                area = number * squared
                mass = area * jnp.sqrt(squared)
                for m, term in enumerate((number, area, mass)):
                    high = term.astype(jnp.bfloat16).astype(jnp.float32)
                    vals[s, k, m * rows:(m + 1) * rows, :] = high
                    vals[s, k, (m + 3) * rows:(m + 4) * rows, :] = term - high
                vals[s, k, 6 * rows:, :] = jnp.zeros((2 * rows, cols), jnp.float32)
            return carry

        loop(levels, cell, 0, 2)

    def clear():
        def level(k, carry):
            acc[k] = jnp.zeros((8 * rows, cols), jnp.float32)
            return carry

        loop(levels + FMAX, level, 0)

    def deposit(begin, end):
        ids = lax.broadcasted_iota(jnp.int32, (cols, cols), 0).astype(jnp.float32).astype(jnp.bfloat16)
        one = jnp.ones((cols, cols), jnp.bfloat16)
        none = jnp.zeros((cols, cols), jnp.bfloat16)
        zero = jnp.zeros((8, cols), jnp.float32)

        def cell(n, carry):
            k, j = begin + n // rows, n % rows
            by_depth = [None] * (FMAX + 1)
            for s in range(0, slots, 4):
                left, hots = [], []
                for t in range(4):
                    v = vals[s + t, k, pl.ds(j, 8, stride=rows), :]
                    left.append(jnp.concatenate([v, zero] if t % 2 == 0 else [zero, v], axis=1))
                    c = column[s + t, k, pl.ds(j, 1), :].astype(jnp.float32).astype(jnp.bfloat16)
                    hots.append(jnp.where(ids == jnp.broadcast_to(c, (cols, cols)), one, none))
                lhs = jnp.concatenate(left, axis=0).astype(jnp.bfloat16)
                rhs = jnp.concatenate(
                    [jnp.concatenate(hots[:2], axis=1), jnp.concatenate(hots[2:], axis=1)], axis=0
                )
                got = lax.dot_general(
                    lhs, rhs, (((1,), (1,)), ((), ())), preferred_element_type=jnp.float32
                )
                for t in range(4):
                    half = t // 2
                    part = got[8 * t:8 * (t + 1), half * cols:(half + 1) * cols]
                    depth = depth_ref[s + t, k * rows + j]
                    for d in range(FMAX + 1):
                        term = jnp.where(depth == d, part, 0.0)
                        by_depth[d] = term if by_depth[d] is None else by_depth[d] + term
            for d in range(FMAX + 1):
                at = pl.ds(pl.multiple_of(j * 8, 8), 8)
                acc[k + FMAX - d, at, :] = acc[k + FMAX - d, at, :] + by_depth[d]
            return carry

        lax.fori_loop(0, (end - begin) * rows, cell, 0, unroll=CELLS)

    def collect(m, l):
        return acc[l, pl.ds(m, rows, stride=8), :] + acc[l, pl.ds(m + 3, rows, stride=8), :]

    copies = max_start(0, top)
    send(0, "0")
    top = max_end(0, top, copies)
    copies = max_start(1, top)
    top = max_end(1, top, copies)
    copies = max_start(2, top)
    clear()
    receive(0, "0")
    advect("0", False)
    receive_y(0, "0")
    advect("0", True)
    top = max_end(2, top, copies)
    time_step = courant_goal / (1.0 + jnp.max(top, axis=(0, 1), keepdims=True))
    time_step = jnp.broadcast_to(time_step, shape)

    third = time_step * (1.0 / 3.0)
    tracer(third)
    substep("0", third)
    send(1, "1")
    receive(1, "1")
    advect("1", False)
    receive_y(1, "1")
    advect("1", True)
    half = time_step * 0.5
    tracer(half)
    part = half / (NS // 2)
    substep("0", part)
    send(2, "1")
    receive(2, "1")
    receive_y(2, "1")
    substep("1", part)
    send(3, "1")
    receive(3, "1")
    advect("1", False)
    receive_y(3, "1")
    advect("1", True)
    tracer(time_step)
    part = time_step / NS
    substep("0", part)
    send(4, "1")
    growth_terms()
    receive(4, "1")
    receive_y(4, "1")
    substep("1", part)
    send(5, "1")
    deposit(0, FMAX)
    moment_copy = pltpu.make_async_remote_copy(
        src_ref=refs["fall_s"], dst_ref=refs["fall_r"],
        send_sem=refs["fall_sem"].at[0], recv_sem=refs["fall_sem"].at[1],
        device_id=neighbour("gz", -1), device_id_type=MESH,
    )
    for m in range(3):
        for l in range(FMAX):
            refs["fall_s"][m, l] = collect(m, l)

    receive(5, "1")
    receive_y(5, "1")

    @pl.when(has_low)
    def _():
        moment_copy.start()

    substep("1", part)
    send(6, "1")
    deposit(FMAX, levels)
    receive(6, "1")
    receive_y(6, "1")
    substep("1", part)

    def write(k, carry):
        out_fields[0, k] = refs["C1"][k + 3]
        out_fields[1, k] = refs["P1"][k + 3]
        out_fields[2, k] = refs["U1"][k]
        out_fields[3, k] = refs["V1"][k]
        out_fields[4, k] = refs["W1"][k + 1]
        return carry

    loop(levels, write, 0)
    for m in range(3):
        for l in range(levels):
            moments[m, l] = collect(m, l + FMAX)

    @pl.when(has_low)
    def _():
        moment_copy.wait_send()

    @pl.when(has_high)
    def _():
        moment_copy.wait_recv()
        for m in range(3):
            for l in range(FMAX):
                at = levels - FMAX + l
                moments[m, at] = moments[m, at] + refs["fall_r"][m, l]


def per_device(fields, radius, weight, column, counts, fall_depth):
    levels, rows, cols = fields.shape[1:]
    slots = radius.shape[0]
    assert slots % 4 == 0 and levels * SLOT_LANES <= cols and rows == 8 and FMAX <= levels
    f32 = jnp.float32
    cell = (rows, cols)
    widest = max(lax.axis_size(a) for a in AXES) - 1
    spaces = {}

    def add(name, *shape, dtype=f32):
        spaces[name] = pltpu.VMEM(shape, dtype)

    add("fields", *fields.shape)
    add("radius", *radius.shape)
    add("weight", *weight.shape)
    add("column", *column.shape, dtype=jnp.int32)
    add("counts", *counts.shape, dtype=jnp.int32)
    for tag in "01":
        add("C" + tag, levels + 6, *cell)
        add("P" + tag, levels + 6, *cell)
        add("U" + tag, levels, *cell)
        add("V" + tag, levels, *cell)
        add("W" + tag, levels + 1, *cell)
        for name in ("HXC", "HXP", "HXU", "HYC", "HYP", "HYV"):
            add(name + tag, levels, *cell)
    add("rate_c", levels, *cell)
    add("rate_p", levels, *cell)
    add("lift", levels + 1, *cell)
    add("max_send", 3, *cell)
    add("max_recv", 3, widest, *cell)
    for end in ("_s", "_r"):
        for name, shape in (
            ("fxu", cell), ("fxd", cell), ("fyu", (levels,) + cell), ("fyd", (levels,) + cell),
            ("fzu", (7,) + cell), ("fzd", (6,) + cell),
        ):
            add(name + end, len(FULL), *shape)
        for name, shape in (
            ("txu", cell), ("txd", cell), ("tyu", (2 * levels, cols)), ("tyd", (levels, cols)),
            ("tzu", (2,) + cell), ("tzd", (1,) + cell),
        ):
            add(name + end, len(THIN), *shape)
    add("acc", levels + FMAX, 8 * rows, cols)
    add("vals", slots, levels, 8 * rows, cols)
    add("fall_s", 3, FMAX, *cell)
    add("fall_r", 3, FMAX, *cell)
    rounds = len(FULL) + len(THIN)
    spaces["send_sem"] = pltpu.SemaphoreType.DMA((rounds, 6))
    spaces["recv_sem"] = pltpu.SemaphoreType.DMA((rounds, 6))
    spaces["max_ss"] = pltpu.SemaphoreType.DMA((3, widest))
    spaces["max_rs"] = pltpu.SemaphoreType.DMA((3, widest))
    spaces["fall_sem"] = pltpu.SemaphoreType.DMA((2,))
    spaces["local_sem"] = pltpu.SemaphoreType.DMA((5,))
    vmem = pl.BlockSpec(memory_space=pltpu.VMEM)
    anywhere = pl.BlockSpec(memory_space=pltpu.HBM)
    return pl.pallas_call(
        functools.partial(kernel, (tuple(spaces), levels, rows, cols, slots)),
        out_shape=(
            jax.ShapeDtypeStruct(fields.shape, f32),
            jax.ShapeDtypeStruct((3, levels, rows, cols), f32),
        ),
        in_specs=[pl.BlockSpec(memory_space=pltpu.SMEM)] + [anywhere] * 5,
        out_specs=(vmem, vmem),
        scratch_shapes=list(spaces.values()),
        compiler_params=pltpu.CompilerParams(
            collective_id=0, has_side_effects=True, vmem_limit_bytes=48 * 1024 * 1024
        ),
        name="slab_step",
    )(fall_depth.reshape(slots, levels * rows), fields, radius, weight, column, counts)


def solution(mesh):
    in_specs = (
        P(None, "gz", "gy", "gx"),
        P(None, "gz", "gy", "gx"),
        P(None, "gz", "gy", "gx"),
        P(None, "gz", "gy", "gx"),
        P("gz", "gy", "gx"),
        P(None, "gz", "gy", "gx"),
    )
    out_specs = (P(None, "gz", "gy", "gx"), P(None, "gz", "gy", "gx"))
    return jax.shard_map(
        per_device, mesh=mesh, in_specs=in_specs, out_specs=out_specs, check_vma=False
    )
```
